32 devices in a mesh: row: 8 (over z, core), col: 4 (over y, x).
Axes of the slice: x: 2, y: 2, z: 4, core: 2. Of those that a mesh axis runs over, the one named last changes fastest.
Arguments:
- act_codes: int32 [512, 7168], P('col', 'row'), may hold values from -127 to 127
- act_scales: float32 [512, 112], P('col', 'row'), may hold values from 0.005 to 0.03
- gate_weight: bfloat16 [7168, 18432], P('row', 'col'), may hold values from -0.0625 to 0.0625
- up_weight: bfloat16 [7168, 18432], P('row', 'col'), may hold values from -0.0625 to 0.0625
- down_weight: bfloat16 [18432, 7168], P('col', 'row'), may hold values from -0.046875 to 0.046875
Outputs:
- mixed: bfloat16 [512, 7168], P('col', 'row')
The draws below stay inside these ranges and needn't reach their ends.
All inputs are finite; a program needn't handle non-finite values.
Results may differ from the reference program's by a relative error of at most 0.03.
Values may be sent and summed in bfloat16 or wider, within the bound.
A program may use at most 128 MiB of HBM per device.

```python
import math
import jax
import jax.numpy as jnp
from jax import lax

D = 7168
FF = 18432
QB = 64
TOKENS = 512
D_ROW = 896
FF_COL = 4608
BLOCKS = 112
N_ROW = 8
N_COL = 4


def place_ends(entries, rng, least, top_value):
    index_at = [jax.random.randint(jax.random.fold_in(rng, axis), (), 0, length) for axis, length in enumerate(entries.shape)]
    widest = entries.shape.index(max(entries.shape))
    next_to = index_at[:widest] + [(index_at[widest] + 1) % entries.shape[widest]] + index_at[widest + 1:]
    return entries.at[tuple(index_at)].set(least).at[tuple(next_to)].set(top_value)


def shard_levels(own_key, dims, cuts, smallest, high):
    loudness, own = 1.0, jax.random.fold_in(own_key, 6)
    for axis_at, blocks in cuts:
        steps = jnp.exp(jax.random.uniform(jax.random.fold_in(own, axis_at), (blocks,), jnp.float32, smallest / len(cuts), high / len(cuts)))
        loudness = loudness * jnp.repeat(steps, dims[axis_at] // blocks).reshape([-1 if axis == axis_at else 1 for axis in range(len(dims))])
    return loudness


def centred(key, extent, width, most, cuts=(), kind=jnp.bfloat16):
    values = jax.random.normal(key, extent, jnp.float32) * width
    if len(cuts) > 0:
        values = shard_levels(key, extent, cuts, -0.22, 0.18) * values
    return jnp.clip(values, min=-most, max=most).astype(kind)


def setup_inputs(seed: int = 0) -> dict:
    keys = jax.random.split(jax.random.key(seed), 6)
    act_codes = place_ends(jax.random.randint(keys[0], (TOKENS, D), -127, 128), jax.random.fold_in(keys[0], 1), -127, 127).astype(jnp.int32)
    act_scales = jnp.clip(jnp.exp(math.log(0.03) - 1.7917595 * jax.random.uniform(keys[1], (TOKENS, BLOCKS), jnp.float32) ** shard_levels(keys[1], (TOKENS, BLOCKS), ((0, 4), (1, 8)), -0.2, 0.2)), 0.005, 0.03)
    gate_weight = centred(keys[2], (D, FF), D ** -0.5, 0.0625, ((0, 8), (1, 4)))
    up_weight = centred(keys[3], (D, FF), D ** -0.5, 0.0625, ((0, 8), (1, 4)))
    down_weight = centred(keys[4], (FF, D), FF ** -0.5, 0.046875, ((0, 4), (1, 8)))
    return dict(act_codes=act_codes, act_scales=act_scales, gate_weight=gate_weight, up_weight=up_weight, down_weight=down_weight)


def dequantize(act_codes, act_scales):
    rows = act_codes.shape[0]
    blocked = act_codes.astype(jnp.float32).reshape(rows, BLOCKS, QB)
    scaled = blocked * act_scales[:, :, None]
    return scaled.reshape(rows, D).astype(jnp.bfloat16)


def rounded(value):
    narrow = lax.optimization_barrier(value.astype(jnp.bfloat16))
    return narrow.astype(jnp.float32)


def reference(act_codes, act_scales, gate_weight, up_weight, down_weight):
    acts = dequantize(act_codes, act_scales)

    def feature_group(index, totals):
        start = (index * D_ROW).astype(jnp.int32)
        slab = lax.dynamic_slice_in_dim(acts, start, D_ROW, 1)
        gate_rows = lax.dynamic_slice_in_dim(gate_weight, start, D_ROW, 0)
        up_rows = lax.dynamic_slice_in_dim(up_weight, start, D_ROW, 0)
        gate_part = rounded(jnp.dot(slab, gate_rows, preferred_element_type=jnp.float32))
        up_part = rounded(jnp.dot(slab, up_rows, preferred_element_type=jnp.float32))
        return (totals[0] + gate_part, totals[1] + up_part)

    empty = jnp.zeros((TOKENS, FF), jnp.float32)
    gate, up = lax.fori_loop(0, N_ROW, feature_group, (empty, empty))
    hidden = (jax.nn.silu(gate) * up).astype(jnp.bfloat16)

    def hidden_group(index, total):
        start = (index * FF_COL).astype(jnp.int32)
        slab = lax.dynamic_slice_in_dim(hidden, start, FF_COL, 1)
        rows_down = lax.dynamic_slice_in_dim(down_weight, start, FF_COL, 0)
        return total + rounded(jnp.dot(slab, rows_down, preferred_element_type=jnp.float32))

    mixed = lax.fori_loop(0, N_COL, hidden_group, jnp.zeros((TOKENS, D), jnp.float32))
    return mixed.astype(jnp.bfloat16)
```

```python
import functools

import jax
import jax.numpy as jnp
from jax import lax
from jax.experimental import pallas as pl
from jax.experimental.pallas import tpu as pltpu
from jax.sharding import PartitionSpec as P

MESH = pl.DeviceIdType.MESH
WIDTHS = (512, 384, 256, 128)
AHEAD = 2
LAG = 28
LAG_HOP = 8
FETCH = 3
EARLY = 2
EARLY_HOP = 3
EARLY_LAST = 3


def body(
    n_row, n_col, codes_hbm, scales_hbm, gate_hbm, up_hbm, down_hbm, o_ref,
    codes, scales, every, up_gate, down_w, part, from_core, from_chip, hid, acc, out_send, out_recv,
    in_sem, w_sem, act_s, act_r, core_s, core_r, chip_s, chip_r, cross_s, cross_r, out_s, out_r,
):
    _, _, half, depth = every.shape
    chunks, _, _, width = up_gate.shape
    steps = n_col * chunks
    n_chip = n_row // 2
    nblocks, tokens = scales.shape
    block = depth // nblocks
    others = (n_col - 1) * chunks
    fetch = min(FETCH, chunks)

    row, col = lax.axis_index("row"), lax.axis_index("col")
    chip, core = row // 2, row % 2
    pos = jnp.where(core == 0, chip, n_chip - 1 - chip)
    ahead_row = row + jnp.where(core == 0, 2, -2)
    behind_row = row - jnp.where(core == 0, 2, -2)
    other_row = chip * 2 + 1 - core
    is_first, is_last = pos == 0, pos == n_chip - 1

    def partner(p):
        there, bit = 0, 1
        while bit < n_col:
            there += bit * lax.rem(col // bit + p // bit, 2)
            bit *= 2
        return there

    def hidden_step(k):
        return jnp.where(k < others, k + chunks, k - others)

    def fetch_up_gate(j):
        columns = pl.ds(j * width, width)
        pltpu.make_async_copy(gate_hbm.at[:, columns], up_gate.at[j, 0], w_sem.at[j]).start()
        pltpu.make_async_copy(up_hbm.at[:, columns], up_gate.at[j, 1], w_sem.at[j]).start()

    def wait_up_gate(j):
        pltpu.make_async_copy(up_gate.at[j], up_gate.at[j], w_sem.at[j]).wait()

    def down_copy(j):
        return pltpu.make_async_copy(down_hbm.at[pl.ds(j * width, width), :], down_w.at[j], w_sem.at[j])

    codes_copy = pltpu.make_async_copy(codes_hbm, codes, in_sem.at[0])
    scales_copy = pltpu.make_async_copy(scales_hbm, scales, in_sem.at[1])
    codes_copy.start()
    scales_copy.start()
    fetch_up_gate(0)

    barrier = pltpu.get_barrier_semaphore()
    for p in range(1, n_col):
        pl.semaphore_signal(barrier, inc=1, device_id={"col": partner(p)}, device_id_type=MESH)
    pl.semaphore_signal(barrier, inc=1, device_id={"row": other_row}, device_id_type=MESH)

    @pl.when(chip > 0)
    def _():
        pl.semaphore_signal(barrier, inc=1, device_id={"row": row - 2}, device_id_type=MESH)

    @pl.when(chip < n_chip - 1)
    def _():
        pl.semaphore_signal(barrier, inc=1, device_id={"row": row + 2}, device_id_type=MESH)

    neighbours = jnp.where(chip > 0, 1, 0) + jnp.where(chip < n_chip - 1, 1, 0)

    def remote(src, dst, send, recv, where):
        return pltpu.make_async_remote_copy(
            src_ref=src, dst_ref=dst, send_sem=send, recv_sem=recv, device_id=where, device_id_type=MESH
        )

    def act_copy(p):
        return remote(every.at[0], every.at[p], act_s, act_r.at[p], {"col": partner(p)})

    def core_copy(j):
        return remote(part.at[j, 1 - core], from_core.at[j], core_s, core_r.at[j], {"row": other_row})

    def chip_copy(j):
        return remote(part.at[j, core], from_chip.at[j], chip_s, chip_r.at[j], {"row": ahead_row})

    def hidden_back(j):
        return remote(hid.at[j, core], hid.at[j, core], chip_s, chip_r.at[j], {"row": behind_row})

    def hidden_across(j):
        return remote(hid.at[j, core], hid.at[j, core], cross_s, cross_r.at[j], {"row": other_row})

    def hidden_crossed(j):
        return remote(hid.at[j, 1 - core], hid.at[j, 1 - core], cross_s, cross_r.at[j], {"row": other_row})

    def out_copy(p):
        return remote(out_send.at[p], out_recv.at[p], out_s, out_r.at[p], {"col": partner(p)})

    def product(j, b, c):
        x = every[b].reshape(2 * half, depth)
        for at in range(2):
            y = jnp.dot(x, up_gate[c, at], preferred_element_type=jnp.float32).astype(jnp.bfloat16)
            part[j, :, :, at * width:(at + 1) * width] = y.reshape(2, half, width)

    codes_copy.wait()
    scales_copy.wait()
    for j in range(1, fetch):
        fetch_up_gate(j)
    by_token = scales[...].T
    for lane in range(0, depth, 128):
        lanes = min(128, depth - lane)
        first = lane // block
        s = by_token[:, first:first + 1]
        at = lax.broadcasted_iota(jnp.int32, (tokens, lanes), 1)
        for k in range(1, lanes // block):
            s = jnp.where(at >= k * block, by_token[:, first + k:first + k + 1], s)
        x = (codes[:, lane:lane + lanes].astype(jnp.float32) * s).astype(jnp.bfloat16)
        every[0, :, :, lane:lane + lanes] = x.reshape(2, half, lanes)
    acc[...] = jnp.zeros_like(acc)

    wait_up_gate(0)
    product(0, 0, 0)

    pl.semaphore_wait(barrier, n_col + neighbours)
    core_copy(0).start()
    for p in range(1, n_col):
        act_copy(p).start()

    def multiply(j):
        b, c = j // chunks, lax.rem(j, chunks)

        @pl.when((b > 0) & (c == 0))
        def _():
            act_copy(b).wait_recv()

        @pl.when(b == 0)
        def _():
            wait_up_gate(c)

            @pl.when(c + fetch - 1 < chunks)
            def _():
                fetch_up_gate(c + fetch - 1)

        @pl.when(b == 1)
        def _():
            down_copy(c).start()

        product(j, b, c)
        core_copy(j).start()

    def add_up(j):
        core_copy(j).wait_recv()

        @pl.when(is_first)
        def _():
            part[j, core] = (
                part[j, core].astype(jnp.float32) + from_core[j].astype(jnp.float32)
            ).astype(jnp.bfloat16)
            chip_copy(j).start()

        @pl.when(jnp.logical_not(is_first))
        def _():
            chip_copy(j).wait_recv()

        @pl.when(jnp.logical_not(is_first) & jnp.logical_not(is_last))
        def _():
            part[j, core] = (
                part[j, core].astype(jnp.float32)
                + from_core[j].astype(jnp.float32)
                + from_chip[j].astype(jnp.float32)
            ).astype(jnp.bfloat16)
            chip_copy(j).start()

        @pl.when(is_last)
        def _():
            def total(lanes):
                return (
                    part[j, core, :, lanes].astype(jnp.float32)
                    + from_core[j, :, lanes].astype(jnp.float32)
                    + from_chip[j, :, lanes].astype(jnp.float32)
                )

            gate, up = total(slice(0, width)), total(slice(width, 2 * width))
            hid[j, core] = (gate / (1.0 + jnp.exp(-gate)) * up).astype(jnp.bfloat16)

    def pass_on(k):
        j = hidden_step(k)

        @pl.when(jnp.logical_not(is_last))
        def _():
            hidden_back(j).wait_recv()

        @pl.when(jnp.logical_not(is_first))
        def _():
            hidden_back(j).start()

        hidden_across(j).start()

    def multiply_down(k):
        j = hidden_step(k)
        c = lax.rem(k, chunks)
        hidden_crossed(j).wait_recv()

        @pl.when(k < chunks)
        def _():
            down_copy(c).wait()

        h = hid[j].reshape(2 * half, width)
        acc[...] += jnp.dot(h, down_w[c], preferred_element_type=jnp.float32)

        @pl.when((k < others) & (c == chunks - 1))
        def _():
            b = k // chunks + 1
            out_send[b] = acc[...].astype(jnp.bfloat16)
            acc[...] = jnp.zeros_like(acc)
            out_copy(b).start()

    lag = LAG + LAG_HOP * (n_chip - 1 - pos)
    down_lag = LAG + LAG_HOP * jnp.maximum(pos, n_chip - 1 - pos) + 2
    early = jnp.minimum(EARLY + EARLY_HOP * pos + jnp.where(is_last, EARLY_LAST, 0), steps)

    def begin(j, carry):
        multiply(j)
        return carry

    lax.fori_loop(1, early, begin, 0)

    def step(i, carry):
        @pl.when(i + early < steps)
        def _():
            multiply(i + early)

        @pl.when(i < steps)
        def _():
            add_up(i)

        @pl.when((i >= lag) & (i - lag < steps))
        def _():
            pass_on(i - lag)

        @pl.when(i >= down_lag)
        def _():
            multiply_down(i - down_lag)

        return carry

    lax.fori_loop(0, steps + down_lag, step, 0)

    total = acc[...]
    for p in range(1, n_col):
        out_copy(p).wait_recv()
        total += out_recv[p].astype(jnp.float32)
    o_ref[...] = total.astype(o_ref.dtype)

    def all_sent(ref, send):
        remote(ref, ref, send, core_r.at[0], {"row": other_row}).wait_send()

    all_sent(from_core, core_s)
    all_sent(hid.at[:, 0], cross_s)

    @pl.when(jnp.logical_not(is_last))
    def _():
        all_sent(from_chip, chip_s)

    @pl.when(jnp.logical_not(is_first))
    def _():
        all_sent(hid.at[:, 0], chip_s)

    all_sent(every.at[pl.ds(1, n_col - 1)], act_s)
    all_sent(out_recv.at[pl.ds(1, n_col - 1)], out_s)


def on_device(n_row, n_col, act_codes, act_scales, gate_weight, up_weight, down_weight):
    tokens, depth = act_codes.shape
    nblocks = act_scales.shape[1]
    hidden, out_width = down_weight.shape
    half = tokens // 2
    width = next(w for w in WIDTHS if hidden % w == 0)
    chunks = hidden // width
    steps = n_col * chunks
    bf16 = jnp.bfloat16
    dma = pltpu.SemaphoreType.DMA
    return pl.pallas_call(
        functools.partial(body, n_row, n_col),
        out_shape=jax.ShapeDtypeStruct((tokens, out_width), bf16),
        in_specs=[pl.BlockSpec(memory_space=pl.ANY)] * 5,
        out_specs=pl.BlockSpec(memory_space=pltpu.VMEM),
        scratch_shapes=[
            pltpu.VMEM((tokens, depth), jnp.int32),
            pltpu.VMEM((nblocks, tokens), jnp.float32),
            pltpu.VMEM((n_col, 2, half, depth), bf16),
            pltpu.VMEM((chunks, 2, depth, width), bf16),
            pltpu.VMEM((chunks, width, out_width), bf16),
            pltpu.VMEM((steps, 2, half, 2 * width), bf16),
            pltpu.VMEM((steps, half, 2 * width), bf16),
            pltpu.VMEM((steps, half, 2 * width), bf16),
            pltpu.VMEM((steps, 2, half, width), bf16),
            pltpu.VMEM((tokens, out_width), jnp.float32),
            pltpu.VMEM((n_col, tokens, out_width), bf16),
            pltpu.VMEM((n_col, tokens, out_width), bf16),
            dma((2,)),
            dma((chunks,)),
            dma,
            dma((n_col,)),
            dma,
            dma((steps,)),
            dma,
            dma((steps,)),
            dma,
            dma((steps,)),
            dma,
            dma((n_col,)),
        ],
        compiler_params=pltpu.CompilerParams(
            collective_id=0, has_side_effects=True, vmem_limit_bytes=67043328
        ),
    )(act_codes, act_scales.T, gate_weight, up_weight, down_weight)


def solution(mesh):
    placed = (P("col", "row"), P("col", "row"), P("row", "col"), P("row", "col"), P("col", "row"))
    return jax.shard_map(
        functools.partial(on_device, mesh.shape["row"], mesh.shape["col"]),
        mesh=mesh,
        in_specs=placed,
        out_specs=P("col", "row"),
        check_vma=False,
    )
```

```python
import functools

import jax
import jax.numpy as jnp
from jax import lax
from jax.experimental import pallas as pl
from jax.experimental.pallas import tpu as pltpu
from jax.sharding import PartitionSpec as P

MESH = pl.DeviceIdType.MESH
WIDTHS = (512, 384, 256, 128)
AHEAD = 2
BEFORE = (8, 3, 0)
DOWN_AFTER = 1
PER_STEP = 2
FETCH = 3
EARLY = 2
EARLY_HOP = 4
EARLY_LAST = 3


def body(
    n_row, n_col, codes_hbm, scales_hbm, gate_hbm, up_hbm, down_hbm, o_ref,
    codes, scales, every, up_gate, down_w, part, from_core, from_chip, hid, acc, out_send, out_recv,
    in_sem, w_sem, act_s, act_r, core_s, core_r, chip_s, chip_r, cross_s, cross_r, out_s, out_r,
):
    _, _, half, depth = every.shape
    chunks, _, _, width = up_gate.shape
    steps = n_col * chunks
    n_chip = n_row // 2
    nblocks, tokens = scales.shape
    block = depth // nblocks
    others = (n_col - 1) * chunks
    fetch = min(FETCH, chunks)

    row, col = lax.axis_index("row"), lax.axis_index("col")
    chip, core = row // 2, row % 2
    pos = jnp.where(core == 0, chip, n_chip - 1 - chip)
    ahead_row = row + jnp.where(core == 0, 2, -2)
    behind_row = row - jnp.where(core == 0, 2, -2)
    other_row = chip * 2 + 1 - core
    is_first, is_last = pos == 0, pos == n_chip - 1

    def partner(p):
        middle = n_col // 2
        p = jnp.where(p < middle, p, jnp.where(p == n_col - 1, middle, p + 1))
        there, bit = 0, 1
        while bit < n_col:
            there += bit * lax.rem(col // bit + p // bit, 2)
            bit *= 2
        return there

    def hidden_step(k):
        return jnp.where(k < others, k + chunks, k - others)

    def fetch_up_gate(j):
        columns = pl.ds(j * width, width)
        pltpu.make_async_copy(gate_hbm.at[:, columns], up_gate.at[j, 0], w_sem.at[j]).start()
        pltpu.make_async_copy(up_hbm.at[:, columns], up_gate.at[j, 1], w_sem.at[j]).start()

    def wait_up_gate(j):
        pltpu.make_async_copy(up_gate.at[j], up_gate.at[j], w_sem.at[j]).wait()

    def down_copy(j):
        return pltpu.make_async_copy(down_hbm.at[pl.ds(j * width, width), :], down_w.at[j], w_sem.at[j])

    codes_copy = pltpu.make_async_copy(codes_hbm, codes, in_sem.at[0])
    scales_copy = pltpu.make_async_copy(scales_hbm, scales, in_sem.at[1])
    codes_copy.start()
    scales_copy.start()
    fetch_up_gate(0)

    barrier = pltpu.get_barrier_semaphore()
    for p in range(1, n_col):
        pl.semaphore_signal(barrier, inc=1, device_id={"col": partner(p)}, device_id_type=MESH)
    pl.semaphore_signal(barrier, inc=1, device_id={"row": other_row}, device_id_type=MESH)

    @pl.when(chip > 0)
    def _():
        pl.semaphore_signal(barrier, inc=1, device_id={"row": row - 2}, device_id_type=MESH)

    @pl.when(chip < n_chip - 1)
    def _():
        pl.semaphore_signal(barrier, inc=1, device_id={"row": row + 2}, device_id_type=MESH)

    neighbours = jnp.where(chip > 0, 1, 0) + jnp.where(chip < n_chip - 1, 1, 0)

    def remote(src, dst, send, recv, where):
        return pltpu.make_async_remote_copy(
            src_ref=src, dst_ref=dst, send_sem=send, recv_sem=recv, device_id=where, device_id_type=MESH
        )

    def act_copy(p):
        return remote(every.at[0], every.at[p], act_s, act_r.at[p], {"col": partner(p)})

    def core_copy(j):
        return remote(part.at[j, 1 - core], from_core.at[j], core_s, core_r.at[j], {"row": other_row})

    def chip_copy(j):
        return remote(part.at[j, core], from_chip.at[j], chip_s, chip_r.at[j], {"row": ahead_row})

    def hidden_back(j):
        return remote(hid.at[j, core], hid.at[j, core], chip_s, chip_r.at[j], {"row": behind_row})

    def hidden_across(j):
        return remote(hid.at[j, core], hid.at[j, core], cross_s, cross_r.at[j], {"row": other_row})

    def hidden_crossed(j):
        return remote(hid.at[j, 1 - core], hid.at[j, 1 - core], cross_s, cross_r.at[j], {"row": other_row})

    def out_copy(p):
        return remote(out_send.at[p], out_recv.at[p], out_s, out_r.at[p], {"col": partner(p)})

    def product(j, b, c):
        x = every[b].reshape(2 * half, depth)
        for at in range(2):
            y = jnp.dot(x, up_gate[c, at], preferred_element_type=jnp.float32).astype(jnp.bfloat16)
            part[j, :, :, at * width:(at + 1) * width] = y.reshape(2, half, width)

    codes_copy.wait()
    scales_copy.wait()
    for j in range(1, fetch):
        fetch_up_gate(j)
    by_token = scales[...].T
    for lane in range(0, depth, 128):
        lanes = min(128, depth - lane)
        first = lane // block
        s = by_token[:, first:first + 1]
        at = lax.broadcasted_iota(jnp.int32, (tokens, lanes), 1)
        for k in range(1, lanes // block):
            s = jnp.where(at >= k * block, by_token[:, first + k:first + k + 1], s)
        x = (codes[:, lane:lane + lanes].astype(jnp.float32) * s).astype(jnp.bfloat16)
        every[0, :, :, lane:lane + lanes] = x.reshape(2, half, lanes)
    acc[...] = jnp.zeros_like(acc)

    wait_up_gate(0)
    product(0, 0, 0)

    pl.semaphore_wait(barrier, n_col + neighbours)
    core_copy(0).start()
    for p in range(1, n_col):
        act_copy(p).start()

    def multiply(j):
        b, c = j // chunks, lax.rem(j, chunks)

        @pl.when((b > 0) & (c == 0))
        def _():
            act_copy(b).wait_recv()

        @pl.when(b == 0)
        def _():
            wait_up_gate(c)

            @pl.when(c + fetch - 1 < chunks)
            def _():
                fetch_up_gate(c + fetch - 1)

        @pl.when(b == 1)
        def _():
            down_copy(c).start()

        product(j, b, c)
        core_copy(j).start()

    def add_up(j):
        core_copy(j).wait_recv()

        @pl.when(is_first)
        def _():
            part[j, core] = (
                part[j, core].astype(jnp.float32) + from_core[j].astype(jnp.float32)
            ).astype(jnp.bfloat16)
            chip_copy(j).start()

        @pl.when(jnp.logical_not(is_first))
        def _():
            chip_copy(j).wait_recv()

        @pl.when(jnp.logical_not(is_first) & jnp.logical_not(is_last))
        def _():
            part[j, core] = (
                part[j, core].astype(jnp.float32)
                + from_core[j].astype(jnp.float32)
                + from_chip[j].astype(jnp.float32)
            ).astype(jnp.bfloat16)
            chip_copy(j).start()

        @pl.when(is_last)
        def _():
            def total(lanes):
                return (
                    part[j, core, :, lanes].astype(jnp.float32)
                    + from_core[j, :, lanes].astype(jnp.float32)
                    + from_chip[j, :, lanes].astype(jnp.float32)
                )

            gate, up = total(slice(0, width)), total(slice(width, 2 * width))
            hid[j, core] = (gate / (1.0 + jnp.exp(-gate)) * up).astype(jnp.bfloat16)

    def pass_on(k):
        j = hidden_step(k)

        @pl.when(jnp.logical_not(is_last))
        def _():
            hidden_back(j).wait_recv()

        @pl.when(jnp.logical_not(is_first))
        def _():
            hidden_back(j).start()

        hidden_across(j).start()

    def multiply_down(k):
        j = hidden_step(k)
        c = lax.rem(k, chunks)
        hidden_crossed(j).wait_recv()

        @pl.when(k < chunks)
        def _():
            down_copy(c).wait()

        h = hid[j].reshape(2 * half, width)
        acc[...] += jnp.dot(h, down_w[c], preferred_element_type=jnp.float32)

        @pl.when((k < others) & (c == chunks - 1))
        def _():
            b = k // chunks + 1
            out_send[b] = acc[...].astype(jnp.bfloat16)
            acc[...] = jnp.zeros_like(acc)
            out_copy(b).start()

    def lag_at(place):
        lag = steps - min(BEFORE[-1], steps // 4)
        for hops, before in enumerate(BEFORE[:-1]):
            lag = jnp.where(place == n_chip - 1 - hops, steps - min(before, steps // 4), lag)
        return lag

    lag = lag_at(pos)
    down_lag = jnp.maximum(lag, lag_at(n_chip - 1 - pos)) + DOWN_AFTER
    early = jnp.minimum(EARLY + EARLY_HOP * pos + jnp.where(is_last, EARLY_LAST, 0), steps)

    def begin(j, carry):
        multiply(j)
        return carry

    lax.fori_loop(1, early, begin, 0)

    def step(i, carry):
        @pl.when(i < steps)
        def _():
            add_up(i)

        @pl.when(i + early < steps)
        def _():
            multiply(i + early)

        for r in range(PER_STEP):
            k = PER_STEP * (i - lag) + r

            @pl.when((k >= 0) & (k < steps))
            def _():
                pass_on(k)

            down = PER_STEP * (i - down_lag) + r

            @pl.when((down >= 0) & (down < steps))
            def _():
                multiply_down(down)

        return carry

    lax.fori_loop(0, down_lag + pl.cdiv(steps, PER_STEP), step, 0)

    total = acc[...]
    for p in range(1, n_col):
        out_copy(p).wait_recv()
        total += out_recv[p].astype(jnp.float32)
    o_ref[...] = total.astype(o_ref.dtype)

    def all_sent(ref, send):
        remote(ref, ref, send, core_r.at[0], {"row": other_row}).wait_send()

    all_sent(from_core, core_s)
    all_sent(hid.at[:, 0], cross_s)

    @pl.when(jnp.logical_not(is_last))
    def _():
        all_sent(from_chip, chip_s)

    @pl.when(jnp.logical_not(is_first))
    def _():
        all_sent(hid.at[:, 0], chip_s)

    all_sent(every.at[pl.ds(1, n_col - 1)], act_s)
    all_sent(out_recv.at[pl.ds(1, n_col - 1)], out_s)


def on_device(n_row, n_col, act_codes, act_scales, gate_weight, up_weight, down_weight):
    tokens, depth = act_codes.shape
    nblocks = act_scales.shape[1]
    hidden, out_width = down_weight.shape
    half = tokens // 2
    width = next(w for w in WIDTHS if hidden % w == 0)
    chunks = hidden // width
    steps = n_col * chunks
    bf16 = jnp.bfloat16
    dma = pltpu.SemaphoreType.DMA
    return pl.pallas_call(
        functools.partial(body, n_row, n_col),
        out_shape=jax.ShapeDtypeStruct((tokens, out_width), bf16),
        in_specs=[pl.BlockSpec(memory_space=pl.ANY)] * 5,
        out_specs=pl.BlockSpec(memory_space=pltpu.VMEM),
        scratch_shapes=[
            pltpu.VMEM((tokens, depth), jnp.int32),
            pltpu.VMEM((nblocks, tokens), jnp.float32),
            pltpu.VMEM((n_col, 2, half, depth), bf16),
            pltpu.VMEM((chunks, 2, depth, width), bf16),
            pltpu.VMEM((chunks, width, out_width), bf16),
            pltpu.VMEM((steps, 2, half, 2 * width), bf16),
            pltpu.VMEM((steps, half, 2 * width), bf16),
            pltpu.VMEM((steps, half, 2 * width), bf16),
            pltpu.VMEM((steps, 2, half, width), bf16),
            pltpu.VMEM((tokens, out_width), jnp.float32),
            pltpu.VMEM((n_col, tokens, out_width), bf16),
            pltpu.VMEM((n_col, tokens, out_width), bf16),
            dma((2,)),
            dma((chunks,)),
            dma,
            dma((n_col,)),
            dma,
            dma((steps,)),
            dma,
            dma((steps,)),
            dma,
            dma((steps,)),
            dma,
            dma((n_col,)),
        ],
        compiler_params=pltpu.CompilerParams(
            collective_id=0, has_side_effects=True, vmem_limit_bytes=67043328
        ),
    )(act_codes, act_scales.T, gate_weight, up_weight, down_weight)


def solution(mesh):
    placed = (P("col", "row"), P("col", "row"), P("row", "col"), P("row", "col"), P("col", "row"))
    return jax.shard_map(
        functools.partial(on_device, mesh.shape["row"], mesh.shape["col"]),
        mesh=mesh,
        in_specs=placed,
        out_specs=P("col", "row"),
        check_vma=False,
    )
```

```python
import functools

import jax
import jax.numpy as jnp
from jax import lax
from jax.experimental import pallas as pl
from jax.experimental.pallas import tpu as pltpu
from jax.sharding import PartitionSpec as P

MESH = pl.DeviceIdType.MESH
WIDTHS = (384, 256, 128)
AHEAD = 2
BEFORE = (9, 4, 1)
DOWN_AFTER = 1
PER_STEP = 2
PER_STEP_LAST = 3
FETCH = 4
EARLY_FIRST = 2
EARLY = 4
EARLY_HOP = 6
EARLY_LAST = 5


def body(
    n_row, n_col, codes_hbm, scales_hbm, gate_hbm, up_hbm, down_hbm, o_ref,
    codes, scales, every, up_gate, down_w, part, from_core, from_chip, hid, acc, out_send, out_recv,
    in_sem, w_sem, act_s, act_r, core_s, core_r, chip_s, chip_r, cross_s, cross_r, out_s, out_r,
):
    _, _, half, depth = every.shape
    chunks, _, _, width = up_gate.shape
    steps = n_col * chunks
    n_chip = n_row // 2
    nblocks, tokens = scales.shape
    block = depth // nblocks
    others = (n_col - 1) * chunks
    fetch = min(FETCH, chunks)

    row, col = lax.axis_index("row"), lax.axis_index("col")
    chip, core = row // 2, row % 2
    pos = jnp.where(core == 0, chip, n_chip - 1 - chip)
    ahead_row = row + jnp.where(core == 0, 2, -2)
    behind_row = row - jnp.where(core == 0, 2, -2)
    other_row = chip * 2 + 1 - core
    is_first, is_last = pos == 0, pos == n_chip - 1

    def partner(p):
        middle = n_col // 2
        p = jnp.where(p < middle, p, jnp.where(p == n_col - 1, middle, p + 1))
        there, bit = 0, 1
        while bit < n_col:
            there += bit * lax.rem(col // bit + p // bit, 2)
            bit *= 2
        return there

    def block_at(turn, side):
        return turn if side == 0 else lax.rem(n_col - turn, n_col)

    def hidden_step(k):
        return jnp.where(k < others, k + chunks, k - others)

    def fetch_up_gate(j):
        columns = pl.ds(j * width, width)
        pltpu.make_async_copy(gate_hbm.at[:, columns], up_gate.at[j, 0], w_sem.at[j]).start()
        pltpu.make_async_copy(up_hbm.at[:, columns], up_gate.at[j, 1], w_sem.at[j]).start()

    def wait_up_gate(j):
        pltpu.make_async_copy(up_gate.at[j], up_gate.at[j], w_sem.at[j]).wait()

    def down_copy(j):
        return pltpu.make_async_copy(down_hbm.at[pl.ds(j * width, width), :], down_w.at[j], w_sem.at[j])

    codes_copy = pltpu.make_async_copy(codes_hbm, codes, in_sem.at[0])
    scales_copy = pltpu.make_async_copy(scales_hbm, scales, in_sem.at[1])
    codes_copy.start()
    scales_copy.start()
    fetch_up_gate(0)

    barrier = pltpu.get_barrier_semaphore()
    for p in range(1, n_col):
        pl.semaphore_signal(barrier, inc=1, device_id={"col": partner(p)}, device_id_type=MESH)
    pl.semaphore_signal(barrier, inc=1, device_id={"row": other_row}, device_id_type=MESH)

    @pl.when(chip > 0)
    def _():
        pl.semaphore_signal(barrier, inc=1, device_id={"row": row - 2}, device_id_type=MESH)

    @pl.when(chip < n_chip - 1)
    def _():
        pl.semaphore_signal(barrier, inc=1, device_id={"row": row + 2}, device_id_type=MESH)

    neighbours = jnp.where(chip > 0, 1, 0) + jnp.where(chip < n_chip - 1, 1, 0)

    def remote(src, dst, send, recv, where):
        return pltpu.make_async_remote_copy(
            src_ref=src, dst_ref=dst, send_sem=send, recv_sem=recv, device_id=where, device_id_type=MESH
        )

    def act_copy(p, side):
        at = 2 * p + side
        return remote(every.at[0, side], every.at[p, side], act_s, act_r.at[at], {"col": partner(p)})

    def core_copy(j):
        return remote(part.at[j, 1 - core], from_core.at[j], core_s, core_r.at[j], {"row": other_row})

    def chip_copy(j):
        return remote(part.at[j, core], from_chip.at[j], chip_s, chip_r.at[j], {"row": ahead_row})

    def hidden_back(j):
        return remote(hid.at[j, core], hid.at[j, core], chip_s, chip_r.at[j], {"row": behind_row})

    def hidden_across(j):
        return remote(hid.at[j, core], hid.at[j, core], cross_s, cross_r.at[j], {"row": other_row})

    def hidden_crossed(j):
        return remote(hid.at[j, 1 - core], hid.at[j, 1 - core], cross_s, cross_r.at[j], {"row": other_row})

    def out_copy(p, side):
        at = 2 * p + side
        return remote(out_send.at[p, side], out_recv.at[p, side], out_s, out_r.at[at], {"col": partner(p)})

    def product(j, turn, c):
        x = jnp.concatenate([every[block_at(turn, side), side] for side in range(2)])
        for at in range(2):
            y = jnp.dot(x, up_gate[c, at], preferred_element_type=jnp.float32).astype(jnp.bfloat16)
            part[j, :, :, at * width:(at + 1) * width] = y.reshape(2, half, width)

    codes_copy.wait()
    scales_copy.wait()
    for j in range(1, fetch):
        fetch_up_gate(j)
    by_token = scales[...].T
    for lane in range(0, depth, 128):
        lanes = min(128, depth - lane)
        first = lane // block
        s = by_token[:, first:first + 1]
        at = lax.broadcasted_iota(jnp.int32, (tokens, lanes), 1)
        for k in range(1, lanes // block):
            s = jnp.where(at >= k * block, by_token[:, first + k:first + k + 1], s)
        x = (codes[:, lane:lane + lanes].astype(jnp.float32) * s).astype(jnp.bfloat16)
        every[0, :, :, lane:lane + lanes] = x.reshape(2, half, lanes)
    acc[...] = jnp.zeros_like(acc)

    wait_up_gate(0)
    product(0, 0, 0)

    pl.semaphore_wait(barrier, n_col + neighbours)
    core_copy(0).start()
    for turn in range(1, n_col):
        for side in range(2):
            act_copy(block_at(turn, side), side).start()

    def multiply(j):
        turn, c = j // chunks, lax.rem(j, chunks)

        @pl.when((turn > 0) & (c == 0))
        def _():
            for side in range(2):
                act_copy(block_at(turn, side), side).wait_recv()

        @pl.when(turn == 0)
        def _():
            wait_up_gate(c)

            @pl.when(c + fetch - 1 < chunks)
            def _():
                fetch_up_gate(c + fetch - 1)

        @pl.when(turn == 1)
        def _():
            down_copy(c).start()

        product(j, turn, c)
        core_copy(j).start()

    def add_up(j):
        core_copy(j).wait_recv()

        @pl.when(is_first)
        def _():
            part[j, core] = (
                part[j, core].astype(jnp.float32) + from_core[j].astype(jnp.float32)
            ).astype(jnp.bfloat16)
            chip_copy(j).start()

        @pl.when(jnp.logical_not(is_first))
        def _():
            chip_copy(j).wait_recv()

        @pl.when(jnp.logical_not(is_first) & jnp.logical_not(is_last))
        def _():
            part[j, core] = (
                part[j, core].astype(jnp.float32)
                + from_core[j].astype(jnp.float32)
                + from_chip[j].astype(jnp.float32)
            ).astype(jnp.bfloat16)
            chip_copy(j).start()

        @pl.when(is_last)
        def _():
            def total(lanes):
                return (
                    part[j, core, :, lanes].astype(jnp.float32)
                    + from_core[j, :, lanes].astype(jnp.float32)
                    + from_chip[j, :, lanes].astype(jnp.float32)
                )

            gate, up = total(slice(0, width)), total(slice(width, 2 * width))
            hid[j, core] = (gate / (1.0 + jnp.exp(-gate)) * up).astype(jnp.bfloat16)

    def send_back(k):
        j = hidden_step(k)
        hidden_back(j).start()
        hidden_across(j).start()

    def pass_on(k):
        j = hidden_step(k)
        hidden_back(j).wait_recv()

        @pl.when(jnp.logical_not(is_first))
        def _():
            hidden_back(j).start()

        hidden_across(j).start()

    def multiply_down(k):
        j = hidden_step(k)
        c = lax.rem(k, chunks)
        hidden_crossed(j).wait_recv()

        @pl.when(k < chunks)
        def _():
            down_copy(c).wait()

        h = hid[j].reshape(2 * half, width)
        acc[...] += jnp.dot(h, down_w[c], preferred_element_type=jnp.float32)

        @pl.when((k < others) & (c == chunks - 1))
        def _():
            for side in range(2):
                b = block_at(k // chunks + 1, side)
                out_send[b, side] = acc[side * half:(side + 1) * half].astype(jnp.bfloat16)
                out_copy(b, side).start()
            acc[...] = jnp.zeros_like(acc)

    def lag_at(place):
        most = (steps - chunks) // PER_STEP_LAST
        lag = steps - min(BEFORE[-1], most)
        for hops, before in enumerate(BEFORE[:-1]):
            lag = jnp.where(place == n_chip - 1 - hops, steps - min(before, most), lag)
        return lag

    lag = lag_at(pos)
    down_lag = jnp.maximum(lag, lag_at(n_chip - 1 - pos)) + DOWN_AFTER
    early = EARLY + EARLY_HOP * (pos - 1) + jnp.where(is_last, EARLY_LAST, 0)
    early = jnp.minimum(jnp.where(is_first, EARLY_FIRST, early), steps)

    def begin(j, carry):
        multiply(j)
        return carry

    lax.fori_loop(1, early, begin, 0)

    def step(i, carry):
        @pl.when(i < steps)
        def _():
            add_up(i)

        @pl.when(i + early < steps)
        def _():
            multiply(i + early)

        for r in range(PER_STEP_LAST):
            k = PER_STEP_LAST * (i - lag) + r

            @pl.when((k >= 0) & (k < steps) & is_last)
            def _():
                send_back(k)

        for r in range(PER_STEP):
            k = PER_STEP * (i - lag) + r

            @pl.when((k >= 0) & (k < steps) & jnp.logical_not(is_last))
            def _():
                pass_on(k)

            down = PER_STEP * (i - down_lag) + r

            @pl.when((down >= 0) & (down < steps))
            def _():
                multiply_down(down)

        return carry

    lax.fori_loop(0, down_lag + pl.cdiv(steps, PER_STEP), step, 0)

    total = acc[...]
    for turn in range(1, n_col):
        for side in range(2):
            out_copy(block_at(turn, side), side).wait_recv()
    for p in range(1, n_col):
        total += out_recv[p].reshape(total.shape).astype(jnp.float32)
    o_ref[...] = total.astype(o_ref.dtype)

    def all_sent(ref, send):
        remote(ref, ref, send, core_r.at[0], {"row": other_row}).wait_send()

    all_sent(from_core, core_s)
    all_sent(hid.at[:, 0], cross_s)

    @pl.when(jnp.logical_not(is_last))
    def _():
        all_sent(from_chip, chip_s)

    @pl.when(jnp.logical_not(is_first))
    def _():
        all_sent(hid.at[:, 0], chip_s)

    all_sent(every.at[pl.ds(1, n_col - 1)], act_s)
    all_sent(out_recv.at[pl.ds(1, n_col - 1)], out_s)


def on_device(n_row, n_col, act_codes, act_scales, gate_weight, up_weight, down_weight):
    tokens, depth = act_codes.shape
    nblocks = act_scales.shape[1]
    hidden, out_width = down_weight.shape
    half = tokens // 2
    width = next(w for w in WIDTHS if hidden % w == 0)
    chunks = hidden // width
    steps = n_col * chunks
    bf16 = jnp.bfloat16
    dma = pltpu.SemaphoreType.DMA
    return pl.pallas_call(
        functools.partial(body, n_row, n_col),
        out_shape=jax.ShapeDtypeStruct((tokens, out_width), bf16),
        in_specs=[pl.BlockSpec(memory_space=pl.ANY)] * 5,
        out_specs=pl.BlockSpec(memory_space=pltpu.VMEM),
        scratch_shapes=[
            pltpu.VMEM((tokens, depth), jnp.int32),
            pltpu.VMEM((nblocks, tokens), jnp.float32),
            pltpu.VMEM((n_col, 2, half, depth), bf16),
            pltpu.VMEM((chunks, 2, depth, width), bf16),
            pltpu.VMEM((chunks, width, out_width), bf16),
            pltpu.VMEM((steps, 2, half, 2 * width), bf16),
            pltpu.VMEM((steps, half, 2 * width), bf16),
            pltpu.VMEM((steps, half, 2 * width), bf16),
            pltpu.VMEM((steps, 2, half, width), bf16),
            pltpu.VMEM((tokens, out_width), jnp.float32),
            pltpu.VMEM((n_col, 2, half, out_width), bf16),
            pltpu.VMEM((n_col, 2, half, out_width), bf16),
            dma((2,)),
            dma((chunks,)),
            dma,
            dma((2 * n_col,)),
            dma,
            dma((steps,)),
            dma,
            dma((steps,)),
            dma,
            dma((steps,)),
            dma,
            dma((2 * n_col,)),
        ],
        compiler_params=pltpu.CompilerParams(
            collective_id=0, has_side_effects=True, vmem_limit_bytes=67043328
        ),
    )(act_codes, act_scales.T, gate_weight, up_weight, down_weight)


def solution(mesh):
    placed = (P("col", "row"), P("col", "row"), P("row", "col"), P("row", "col"), P("col", "row"))
    return jax.shard_map(
        functools.partial(on_device, mesh.shape["row"], mesh.shape["col"]),
        mesh=mesh,
        in_specs=placed,
        out_specs=P("col", "row"),
        check_vma=False,
    )
```

```python
import functools

import jax
import jax.numpy as jnp
from jax import lax
from jax.experimental import pallas as pl
from jax.experimental.pallas import tpu as pltpu
from jax.sharding import PartitionSpec as P

MESH = pl.DeviceIdType.MESH
WIDTHS = (384, 256, 128)
AHEAD = 2
BEFORE = (9, 4, 1)
DOWN_AFTER = 1
PER_STEP = 2
PER_STEP_LAST = 3
FETCH = 4
EARLY_FIRST = 2
EARLY = 4
EARLY_HOP = 6
EARLY_LAST = 5


def body(
    n_row, n_col, codes_hbm, scales_hbm, gate_hbm, up_hbm, down_hbm, o_ref,
    codes, scales, every, up_gate, down_w, part, from_core, from_chip, hid, acc, out_send, out_recv,
    in_sem, w_sem, act_s, act_r, core_s, chip_s, chip_r, cross_s, cross_r, out_s, out_r,
):
    _, _, half, depth = every.shape
    chunks, _, _, width = up_gate.shape
    steps = n_col * chunks
    n_chip = n_row // 2
    nblocks, tokens = scales.shape
    block = depth // nblocks
    others = (n_col - 1) * chunks
    fetch = min(FETCH, chunks)

    row, col = lax.axis_index("row"), lax.axis_index("col")
    chip, core = row // 2, row % 2
    pos = jnp.where(core == 0, chip, n_chip - 1 - chip)
    ahead_row = row + jnp.where(core == 0, 2, -2)
    behind_row = row - jnp.where(core == 0, 2, -2)
    other_row = chip * 2 + 1 - core
    is_first, is_last = pos == 0, pos == n_chip - 1

    def partner(p):
        middle = n_col // 2
        p = jnp.where(p < middle, p, jnp.where(p == n_col - 1, middle, p + 1))
        there, bit = 0, 1
        while bit < n_col:
            there += bit * lax.rem(col // bit + p // bit, 2)
            bit *= 2
        return there

    def block_at(turn, side):
        return turn if side == 0 else lax.rem(n_col - turn, n_col)

    def hidden_step(k):
        return jnp.where(k < others, k + chunks, k - others)

    def fetch_up_gate(j):
        columns = pl.ds(j * width, width)
        pltpu.make_async_copy(gate_hbm.at[:, columns], up_gate.at[j, 0], w_sem.at[j]).start()
        pltpu.make_async_copy(up_hbm.at[:, columns], up_gate.at[j, 1], w_sem.at[j]).start()

    def wait_up_gate(j):
        pltpu.make_async_copy(up_gate.at[j], up_gate.at[j], w_sem.at[j]).wait()

    def down_copy(j):
        return pltpu.make_async_copy(down_hbm.at[pl.ds(j * width, width), :], down_w.at[j], w_sem.at[j])

    codes_copy = pltpu.make_async_copy(codes_hbm, codes, in_sem.at[0])
    scales_copy = pltpu.make_async_copy(scales_hbm, scales, in_sem.at[1])
    codes_copy.start()
    scales_copy.start()
    fetch_up_gate(0)

    barrier = pltpu.get_barrier_semaphore()
    for p in range(1, n_col):
        pl.semaphore_signal(barrier, inc=1, device_id={"col": partner(p)}, device_id_type=MESH)
    pl.semaphore_signal(barrier, inc=1, device_id={"row": other_row}, device_id_type=MESH)

    @pl.when(chip > 0)
    def _():
        pl.semaphore_signal(barrier, inc=1, device_id={"row": row - 2}, device_id_type=MESH)

    @pl.when(chip < n_chip - 1)
    def _():
        pl.semaphore_signal(barrier, inc=1, device_id={"row": row + 2}, device_id_type=MESH)

    neighbours = jnp.where(chip > 0, 1, 0) + jnp.where(chip < n_chip - 1, 1, 0)

    def remote(src, dst, send, recv, where):
        return pltpu.make_async_remote_copy(
            src_ref=src, dst_ref=dst, send_sem=send, recv_sem=recv, device_id=where, device_id_type=MESH
        )

    def act_copy(p, side):
        at = 2 * p + side
        return remote(every.at[0, side], every.at[p, side], act_s, act_r.at[at], {"col": partner(p)})

    def core_copy(j):
        return remote(part.at[j, 1 - core], from_core.at[j], core_s, chip_r.at[j], {"row": other_row})

    def chip_copy(j):
        return remote(part.at[j, core], from_chip.at[j], chip_s, chip_r.at[j], {"row": ahead_row})

    def hidden_back(j):
        return remote(hid.at[j, core], hid.at[j, core], chip_s, chip_r.at[j], {"row": behind_row})

    def hidden_across(j):
        return remote(hid.at[j, core], hid.at[j, core], cross_s, cross_r.at[j], {"row": other_row})

    def hidden_crossed(j):
        return remote(hid.at[j, 1 - core], hid.at[j, 1 - core], cross_s, cross_r.at[j], {"row": other_row})

    def out_copy(p, side):
        at = 2 * p + side
        return remote(out_send.at[p, side], out_recv.at[p, side], out_s, out_r.at[at], {"col": partner(p)})

    def product(j, turn, c):
        x = jnp.concatenate([every[block_at(turn, side), side] for side in range(2)])
        for at in range(2):
            y = jnp.dot(x, up_gate[c, at], preferred_element_type=jnp.float32).astype(jnp.bfloat16)
            part[j, :, :, at * width:(at + 1) * width] = y.reshape(2, half, width)

    codes_copy.wait()
    scales_copy.wait()
    for j in range(1, fetch):
        fetch_up_gate(j)
    by_token = scales[...].T
    for lane in range(0, depth, 128):
        lanes = min(128, depth - lane)
        first = lane // block
        s = by_token[:, first:first + 1]
        at = lax.broadcasted_iota(jnp.int32, (tokens, lanes), 1)
        for k in range(1, lanes // block):
            s = jnp.where(at >= k * block, by_token[:, first + k:first + k + 1], s)
        x = (codes[:, lane:lane + lanes].astype(jnp.float32) * s).astype(jnp.bfloat16)
        every[0, :, :, lane:lane + lanes] = x.reshape(2, half, lanes)
    acc[...] = jnp.zeros_like(acc)

    wait_up_gate(0)
    product(0, 0, 0)

    pl.semaphore_wait(barrier, n_col + neighbours)
    core_copy(0).start()
    for turn in range(1, n_col):
        for side in range(2):
            act_copy(block_at(turn, side), side).start()

    def multiply(j):
        turn, c = j // chunks, lax.rem(j, chunks)

        @pl.when((turn > 0) & (c == 0))
        def _():
            for side in range(2):
                act_copy(block_at(turn, side), side).wait_recv()

        @pl.when(turn == 0)
        def _():
            wait_up_gate(c)

            @pl.when(c + fetch - 1 < chunks)
            def _():
                fetch_up_gate(c + fetch - 1)

        @pl.when(turn == 1)
        def _():
            down_copy(c).start()

        product(j, turn, c)
        core_copy(j).start()

    def add_up(j):
        @pl.when(is_first)
        def _():
            core_copy(j).wait_recv()
            part[j, core] = (
                part[j, core].astype(jnp.float32) + from_core[j].astype(jnp.float32)
            ).astype(jnp.bfloat16)
            chip_copy(j).start()

        @pl.when(jnp.logical_not(is_first))
        def _():
            remote(part.at[j], part.at[j], core_s, chip_r.at[j], {"row": other_row}).wait_recv()

        @pl.when(jnp.logical_not(is_first) & jnp.logical_not(is_last))
        def _():
            part[j, core] = (
                part[j, core].astype(jnp.float32)
                + from_core[j].astype(jnp.float32)
                + from_chip[j].astype(jnp.float32)
            ).astype(jnp.bfloat16)
            chip_copy(j).start()

        @pl.when(is_last)
        def _():
            def total(lanes):
                return (
                    part[j, core, :, lanes].astype(jnp.float32)
                    + from_core[j, :, lanes].astype(jnp.float32)
                    + from_chip[j, :, lanes].astype(jnp.float32)
                )

            gate, up = total(slice(0, width)), total(slice(width, 2 * width))
            hid[j, core] = (gate / (1.0 + jnp.exp(-gate)) * up).astype(jnp.bfloat16)

    def send_back(k):
        j = hidden_step(k)
        hidden_back(j).start()
        hidden_across(j).start()

    def pass_on(k):
        j = hidden_step(k)
        hidden_back(j).wait_recv()

        @pl.when(jnp.logical_not(is_first))
        def _():
            hidden_back(j).start()

        hidden_across(j).start()

    def multiply_down(k):
        j = hidden_step(k)
        c = lax.rem(k, chunks)
        hidden_crossed(j).wait_recv()

        @pl.when(k < chunks)
        def _():
            down_copy(c).wait()

        @pl.when(k == steps - min(2, chunks))
        def _():
            for turn in range(1, n_col):
                for side in range(2):
                    out_copy(block_at(turn, side), side).wait_recv()
            total = acc[...]
            for p in range(1, n_col):
                total += out_recv[p].reshape(total.shape).astype(jnp.float32)
            acc[...] = total

        h = hid[j].reshape(2 * half, width)
        acc[...] += jnp.dot(h, down_w[c], preferred_element_type=jnp.float32)

        @pl.when((k < others) & (c == chunks - 1))
        def _():
            for side in range(2):
                b = block_at(k // chunks + 1, side)
                out_send[b, side] = acc[side * half:(side + 1) * half].astype(jnp.bfloat16)
                out_copy(b, side).start()
            acc[...] = jnp.zeros_like(acc)

    def lag_at(place):
        most = (steps - chunks) // PER_STEP_LAST
        lag = steps - min(BEFORE[-1], most)
        for hops, before in enumerate(BEFORE[:-1]):
            lag = jnp.where(place == n_chip - 1 - hops, steps - min(before, most), lag)
        return lag

    lag = lag_at(pos)
    down_lag = jnp.maximum(lag, lag_at(n_chip - 1 - pos)) + DOWN_AFTER
    early = EARLY + EARLY_HOP * (pos - 1) + jnp.where(is_last, EARLY_LAST, 0)
    early = jnp.minimum(jnp.where(is_first, EARLY_FIRST, early), steps)

    def begin(j, carry):
        multiply(j)
        return carry

    lax.fori_loop(1, early, begin, 0)

    def step(i, carry):
        @pl.when(i < steps)
        def _():
            add_up(i)

        @pl.when(i + early < steps)
        def _():
            multiply(i + early)

        for r in range(PER_STEP_LAST):
            k = PER_STEP_LAST * (i - lag) + r

            @pl.when((k >= 0) & (k < steps) & is_last)
            def _():
                send_back(k)

        for r in range(PER_STEP):
            k = PER_STEP * (i - lag) + r

            @pl.when((k >= 0) & (k < steps) & jnp.logical_not(is_last))
            def _():
                pass_on(k)

            down = PER_STEP * (i - down_lag) + r

            @pl.when((down >= 0) & (down < steps))
            def _():
                multiply_down(down)

        return carry

    lax.fori_loop(0, down_lag + pl.cdiv(steps, PER_STEP), step, 0)

    o_ref[...] = acc[...].astype(o_ref.dtype)

    def all_sent(ref, send):
        remote(ref, ref, send, chip_r.at[0], {"row": other_row}).wait_send()

    all_sent(from_core, core_s)
    all_sent(hid.at[:, 0], cross_s)

    @pl.when(jnp.logical_not(is_last))
    def _():
        all_sent(from_chip, chip_s)

    @pl.when(jnp.logical_not(is_first))
    def _():
        all_sent(hid.at[:, 0], chip_s)

    all_sent(every.at[pl.ds(1, n_col - 1)], act_s)
    all_sent(out_recv.at[pl.ds(1, n_col - 1)], out_s)


def on_device(n_row, n_col, act_codes, act_scales, gate_weight, up_weight, down_weight):
    tokens, depth = act_codes.shape
    nblocks = act_scales.shape[1]
    hidden, out_width = down_weight.shape
    half = tokens // 2
    width = next(w for w in WIDTHS if hidden % w == 0)
    chunks = hidden // width
    steps = n_col * chunks
    bf16 = jnp.bfloat16
    dma = pltpu.SemaphoreType.DMA
    return pl.pallas_call(
        functools.partial(body, n_row, n_col),
        out_shape=jax.ShapeDtypeStruct((tokens, out_width), bf16),
        in_specs=[pl.BlockSpec(memory_space=pl.ANY)] * 5,
        out_specs=pl.BlockSpec(memory_space=pltpu.VMEM),
        scratch_shapes=[
            pltpu.VMEM((tokens, depth), jnp.int32),
            pltpu.VMEM((nblocks, tokens), jnp.float32),
            pltpu.VMEM((n_col, 2, half, depth), bf16),
            pltpu.VMEM((chunks, 2, depth, width), bf16),
            pltpu.VMEM((chunks, width, out_width), bf16),
            pltpu.VMEM((steps, 2, half, 2 * width), bf16),
            pltpu.VMEM((steps, half, 2 * width), bf16),
            pltpu.VMEM((steps, half, 2 * width), bf16),
            pltpu.VMEM((steps, 2, half, width), bf16),
            pltpu.VMEM((tokens, out_width), jnp.float32),
            pltpu.VMEM((n_col, 2, half, out_width), bf16),
            pltpu.VMEM((n_col, 2, half, out_width), bf16),
            dma((2,)),
            dma((chunks,)),
            dma,
            dma((2 * n_col,)),
            dma,
            dma,
            dma((steps,)),
            dma,
            dma((steps,)),
            dma,
            dma((2 * n_col,)),
        ],
        compiler_params=pltpu.CompilerParams(
            collective_id=0, has_side_effects=True, vmem_limit_bytes=67043328
        ),
    )(act_codes, act_scales.T, gate_weight, up_weight, down_weight)


def solution(mesh):
    placed = (P("col", "row"), P("col", "row"), P("row", "col"), P("row", "col"), P("col", "row"))
    return jax.shard_map(
        functools.partial(on_device, mesh.shape["row"], mesh.shape["col"]),
        mesh=mesh,
        in_specs=placed,
        out_specs=P("col", "row"),
        check_vma=False,
    )
```
